32 devices in a mesh: rep: 4 (over y, core), shard: 8 (over z, x).
Axes of the slice: x: 2, y: 2, z: 4, core: 2. Of those that a mesh axis runs over, the one named last changes fastest.
Arguments:
- delta: bfloat16 [4, 512, 6144], P('rep', 'shard'), may hold values from -11 to 11
- counts: int32 [4], replicated, may hold values from 1000 to 7999
- params: bfloat16 [512, 6144], P('shard'), may hold values from -0.078125 to 0.078125
- momentum: float32 [512, 6144], P('shard', 'rep'), may hold values from -4 to 4
Outputs:
- new_params: bfloat16 [512, 6144], P('shard')
- new_momentum: float32 [512, 6144], P('shard', 'rep')
- update_rms: float32 [], replicated
- mean_variance: float32 [], replicated
The draws below stay inside these ranges and needn't reach their ends.
All inputs are finite; a program needn't handle non-finite values.
Results may differ from the reference program's by a relative error of at most 0.0004.
Values may be sent and summed in bfloat16 or wider, within the bound.
A program may use at most 64 MiB of HBM per device.

```python
import jax
import jax.numpy as jnp

D = 6144
ROWS_DEV = 64
ROWS = 512
N_REP = 4


def draw_delta(key, part):
    first_key = jax.random.fold_in(key, 0)
    row_key = jax.random.fold_in(key, 3)
    block_key = jax.random.fold_in(key, 4)
    row_scale = jnp.exp(jax.random.uniform(row_key, (ROWS,), jnp.float32, -1.0, 1.0))
    block_count = ROWS // ROWS_DEV
    column_width = D // N_REP
    block_factor = jnp.exp(jax.random.uniform(block_key, (N_REP, block_count, N_REP), jnp.float32, -0.7, 0.7))
    values = jax.random.truncated_normal(first_key, -6.0, 6.0, (N_REP, ROWS, D), jnp.float32)
    values = values * row_scale[None, :, None]
    shaped = values.reshape(N_REP, block_count, ROWS_DEV, N_REP, column_width)
    shaped = shaped * block_factor[:, :, None, :, None]
    values = jnp.clip(shaped.reshape(N_REP, ROWS, D), -11.0, 11.0)
    return values.astype(jnp.bfloat16)


def touch_ends(array, rng, low, top_value):
    index_at = [jax.random.randint(jax.random.fold_in(rng, axis), (), 0, length) for axis, length in enumerate(array.shape)]
    widest = array.shape.index(max(array.shape))
    next_to = index_at[:widest] + [(index_at[widest] + 1) % array.shape[widest]] + index_at[widest + 1:]
    return array.at[tuple(index_at)].set(low).at[tuple(next_to)].set(top_value)


def steps_of(own_key, dims, pieces, least, largest):
    def one(dim, blocks):
        heights = jax.random.uniform(jax.random.fold_in(jax.random.fold_in(own_key, 6), dim), (blocks,), jnp.float32, least / len(pieces), largest / len(pieces))
        return jnp.repeat(jnp.exp(heights), dims[dim] // blocks).reshape((-1,) + (1,) * (len(dims) - dim - 1))

    level = one(*pieces[0])
    for cut in pieces[1:]:
        level = level * one(*cut)
    return level


def normal_values(stream_key, dims, width, most, shards=(), held_as=jnp.bfloat16):
    drawn = jax.random.normal(stream_key, dims, jnp.float32) * width
    if len(shards) > 0:
        drawn = steps_of(stream_key, dims, shards, -0.22, 0.18) * drawn
    return jnp.clip(drawn, min=-most, max=most).astype(held_as)


def setup_inputs(seed: int = 0) -> dict:
    key_list = jax.random.split(jax.random.key(seed), 5)
    delta = draw_delta(jax.random.fold_in(key_list[4], 71), 0)
    counts = touch_ends(jax.random.randint(key_list[1], (N_REP,), 1000, 8000), jax.random.fold_in(key_list[1], 1), 1000, 7999).astype(jnp.int32)
    params = normal_values(key_list[2], (ROWS, D), D ** -0.5, 0.078125, ((0, 8),))
    momentum = normal_values(key_list[3], (ROWS, D), 0.3, 4.0, ((0, 8), (1, 4)), jnp.float32)
    return dict(delta=delta, counts=counts, params=params, momentum=momentum)


clip_rms = 0.2
beta_outer = 0.9
outer_rate = 0.7
epsilon = 1e-06

def reference(delta, counts, params, momentum):
    tokens = counts.astype(jnp.float32)
    weights = tokens / jnp.sum(tokens)
    mean_delta = jnp.zeros((ROWS, D), jnp.float32)
    for replica in range(N_REP):
        mean_delta = mean_delta + weights[replica] * delta[replica].astype(jnp.float32)
    variance = jnp.zeros((ROWS, D), jnp.float32)
    for replica in range(N_REP):
        centered = delta[replica].astype(jnp.float32) - mean_delta
        variance = variance + weights[replica] * centered * centered
    element_count = ROWS * D
    update_rms = jnp.sqrt(jnp.sum(mean_delta * mean_delta) / element_count)
    mean_variance = jnp.sum(variance) / element_count
    clip_factor = clip_rms / jnp.maximum(update_rms, clip_rms)
    damped = clip_factor * mean_delta / (1.0 + variance / (mean_variance + epsilon))
    new_momentum = beta_outer * momentum + damped
    outer_update = outer_rate * (damped + beta_outer * new_momentum)
    new_params = (params.astype(jnp.float32) - outer_update).astype(jnp.bfloat16)
    return (new_params, new_momentum, update_rms, mean_variance)
```

```python
import functools

import jax
import jax.numpy as jnp
from jax import lax
from jax.experimental import pallas as pl
from jax.experimental.pallas import tpu as pltpu
from jax.sharding import PartitionSpec as P

clip_rms = 0.2
beta_outer = 0.9
outer_rate = 0.7
epsilon = 1e-06

MESH = pl.DeviceIdType.MESH
STEP_ROWS = 16
STEP_COLS = 512
UNROLL_MOST = 64


def kernel(
    n_rep, n_shard, element_count,
    delta_ref, counts_ref, params_ref, momentum_ref,
    new_params_ref, new_momentum_ref, rms_ref, mean_var_ref,
    staged, arrived, mean_buf, var_buf, own_params, own_momentum, sums, tokens,
    stage_sem, local_sem, send_sem, recv_sem, sum_send_sem, sum_recv_sem, out_send_sem, out_recv_sem, round_sem,
):
    rep = lax.axis_index("rep")
    shard = lax.axis_index("shard")
    n_all = n_rep * n_shard
    me = rep * n_shard + shard
    rows, width = own_momentum.shape
    n_steps = rows // STEP_ROWS

    def column_block(index):
        return pl.ds(pl.multiple_of(index * width, 128), width)

    def row_block(step):
        return pl.ds(step * STEP_ROWS, STEP_ROWS)

    def stage(step):
        return pltpu.make_async_copy(
            delta_ref.at[0, row_block(step)], staged.at[row_block(step)], stage_sem.at[step]
        )

    def device_at(offset):
        other = lax.rem(me + offset, n_all)
        return (other // n_shard, lax.rem(other, n_shard))

    barrier = pltpu.get_barrier_semaphore()
    inner = 2 if n_shard % 2 == 0 else 1
    n_outer = n_shard // inner
    outer = shard // inner

    def along_shard(offset):
        return (rep, lax.rem(shard + offset, n_shard))

    def across_rep(hop):
        return (lax.rem(rep + hop, n_rep), shard)

    def signal_line(semaphore, distance):
        for at in (outer + distance, outer - distance):

            @pl.when((at >= 0) & (at < n_outer))
            def _():
                device = (rep, at * inner + lax.rem(shard, inner))
                pl.semaphore_signal(semaphore, inc=1, device_id=device, device_id_type=MESH)

    def on_line(distance):
        return (outer + distance < n_outer).astype(jnp.int32) + (outer >= distance).astype(jnp.int32)

    for hop in range(1, n_rep):
        pl.semaphore_signal(barrier, inc=1, device_id=across_rep(hop), device_id_type=MESH)
    if inner == 2:
        beside = (rep, shard + 1 - 2 * lax.rem(shard, 2))
        pl.semaphore_signal(barrier, inc=1, device_id=beside, device_id_type=MESH)
    if n_outer > 1:
        signal_line(barrier, 1)

    for step in range(n_steps):
        stage(step).start()
    load_counts = pltpu.make_async_copy(counts_ref, tokens, local_sem.at[2])
    load_counts.start()
    load_params = pltpu.make_async_copy(params_ref.at[:, column_block(rep)], own_params, local_sem.at[0])
    load_momentum = pltpu.make_async_copy(momentum_ref, own_momentum, local_sem.at[1])

    near = n_rep - 1 + inner - 1
    pl.semaphore_wait(barrier, near + on_line(1) if n_outer > 1 else near)

    def exchange(step, hop):
        peer = lax.rem(rep + hop, n_rep)
        return pltpu.make_async_remote_copy(
            src_ref=staged.at[row_block(step), column_block(peer)],
            dst_ref=arrived.at[hop - 1, row_block(step)],
            send_sem=send_sem.at[step, hop - 1],
            recv_sem=recv_sem.at[step, hop - 1],
            device_id=(peer, shard),
            device_id_type=MESH,
        )

    for step in range(n_steps):
        stage(step).wait()
        for hop in range(1, n_rep):
            exchange(step, hop).start()

    load_params.start()
    load_momentum.start()

    known = 1
    level = 0
    while known < n_outer - 1:
        signal_line(round_sem.at[level], known)
        pl.semaphore_wait(round_sem.at[level], on_line(known))
        known, level = 2 * known, level + 1
    for hop in range(1, n_rep):
        pl.semaphore_signal(round_sem.at[level], inc=1, device_id=across_rep(hop), device_id_type=MESH)
    pl.semaphore_wait(round_sem.at[level], n_rep - 1)

    tile = (8, 128)
    load_counts.wait()
    total = tokens[0]
    for index in range(1, n_rep):
        total = total + tokens[index]
    total_tokens = jnp.full(tile, total.astype(jnp.float32))

    def weight_of(index):
        return (jnp.full(tile, tokens[index].astype(jnp.float32)) / total_tokens)[0:1, 0:1]

    weights = [weight_of(lax.rem(rep + n_rep - hop, n_rep)) for hop in range(n_rep)]

    square_sum = jnp.zeros(tile, jnp.float32)
    var_sum = jnp.zeros(tile, jnp.float32)
    for step in range(n_steps):
        for hop in range(1, n_rep):
            exchange(step, hop).wait_recv()

        def moments(index, carry):
            square_sum, var_sum = carry
            start = pl.multiple_of(index * STEP_COLS, 128)
            columns = pl.ds(start, STEP_COLS)
            own_columns = pl.ds(pl.multiple_of(rep * width + start, 128), STEP_COLS)
            values = [staged[row_block(step), own_columns].astype(jnp.float32)]
            for hop in range(1, n_rep):
                values.append(arrived[hop - 1, row_block(step), columns].astype(jnp.float32))
            mean = weights[0] * values[0]
            for weight, value in zip(weights[1:], values[1:]):
                mean = mean + weight * value
            variance = jnp.zeros_like(mean)
            for weight, value in zip(weights, values):
                centered = value - mean
                variance = variance + weight * (centered * centered)
            mean_buf[row_block(step), columns] = mean
            var_buf[row_block(step), columns] = variance

            def fold(array):
                out = jnp.zeros(tile, jnp.float32)
                for top in range(0, STEP_ROWS, 8):
                    for left in range(0, STEP_COLS, 128):
                        out = out + array[top:top + 8, left:left + 128]
                return out

            return square_sum + fold(mean * mean), var_sum + fold(variance)

        square_sum, var_sum = lax.fori_loop(0, width // STEP_COLS, moments, (square_sum, var_sum), unroll=True)

    square_row = jnp.sum(square_sum, axis=0, keepdims=True)
    var_row = jnp.sum(var_sum, axis=0, keepdims=True)
    first_half = lax.broadcasted_iota(jnp.int32, (1, 128), 1) < 64
    sums[me] = jnp.where(first_half, square_row + pltpu.roll(square_row, 64, 1), var_row + pltpu.roll(var_row, 64, 1))

    def send_sums(device):
        pltpu.make_async_remote_copy(
            src_ref=sums.at[me],
            dst_ref=sums.at[me],
            send_sem=sum_send_sem,
            recv_sem=sum_recv_sem,
            device_id=device,
            device_id_type=MESH,
        ).start()

    if n_all <= UNROLL_MOST:
        offsets = [(hop, offset) for offset in range(n_shard) for hop in range(n_rep) if hop or offset]
        offsets.sort(key=lambda at: -min(at[1], n_shard - at[1]) - min(at[0], n_rep - at[0]))
        for hop, offset in offsets:
            send_sums((across_rep(hop)[0], along_shard(offset)[1]))
    else:

        @pl.loop(1, n_all)
        def _(offset):
            send_sums(device_at(offset))

    load_params.wait()
    load_momentum.wait()
    others = sums.at[pl.ds(0, n_all - 1)]
    pltpu.make_async_copy(others, others, sum_recv_sem).wait()

    totals = jnp.sum(sums[...], axis=0)
    rms = jnp.sqrt(jnp.sum(jnp.where(first_half, totals, 0.0), axis=1, keepdims=True) / element_count)
    mean_var = jnp.sum(jnp.where(first_half, 0.0, totals), axis=1, keepdims=True) / element_count
    clip_factor = clip_rms / jnp.maximum(rms, clip_rms)
    inverse = 1.0 / (mean_var + epsilon)

    partner = rep + 1 - 2 * lax.rem(rep, 2)
    n_pairs = n_rep // 2

    def send_block(step, owner, target, slot):
        block = new_params_ref.at[row_block(step), column_block(owner)]
        return pltpu.make_async_remote_copy(
            src_ref=block,
            dst_ref=block,
            send_sem=out_send_sem.at[step, slot],
            recv_sem=out_recv_sem.at[step, slot],
            device_id=(target, shard),
            device_id_type=MESH,
        )

    def arriving(step, owner, slot):
        block = new_params_ref.at[row_block(step), column_block(owner)]
        return pltpu.make_async_copy(block, block, out_recv_sem.at[step, slot])

    def to_pair(step, pair):
        return send_block(step, rep, lax.rem(rep + 2 * pair, n_rep), pair - 1)

    def from_pair(step, pair):
        return arriving(step, lax.rem(rep + n_rep - 2 * pair, n_rep), pair - 1)

    def to_partner(step, pair):
        return send_block(step, lax.rem(rep + n_rep - 2 * pair, n_rep), partner, n_pairs - 1 + pair)

    def from_partner(step, pair):
        return arriving(step, lax.rem(partner + n_rep - 2 * pair, n_rep), n_pairs - 1 + pair)

    for step in range(n_steps):

        @pl.loop(0, width // STEP_COLS, unroll=True)
        def _(index):
            start = pl.multiple_of(index * STEP_COLS, 128)
            columns = pl.ds(start, STEP_COLS)
            own_columns = pl.ds(pl.multiple_of(rep * width + start, 128), STEP_COLS)
            mean = mean_buf[row_block(step), columns]
            variance = var_buf[row_block(step), columns]
            damped = clip_factor * mean / (1.0 + variance * inverse)
            new_momentum = beta_outer * own_momentum[row_block(step), columns] + damped
            new_momentum_ref[row_block(step), columns] = new_momentum
            update = outer_rate * (damped + beta_outer * new_momentum)
            old = own_params[row_block(step), columns].astype(jnp.float32)
            new_params_ref[row_block(step), own_columns] = (old - update).astype(jnp.bfloat16)

        for pair in range(1, n_pairs):
            to_pair(step, pair).start()
        to_partner(step, 0).start()

    rms_ref[0] = rms[0, 0]
    mean_var_ref[0] = mean_var[0, 0]
    for step in range(n_steps):
        for pair in range(1, n_pairs):
            from_pair(step, pair).wait()
            to_partner(step, pair).start()
    for step in range(n_steps):
        for hop in range(1, n_rep):
            exchange(step, hop).wait_send()
    pltpu.make_async_copy(others, others, sum_send_sem).wait()
    for step in range(n_steps):
        for pair in range(n_pairs):
            if pair:
                to_pair(step, pair).wait_send()
            to_partner(step, pair).wait_send()
            from_partner(step, pair).wait()


def store(params_ref, momentum_ref, rms_in, mean_var_in, params_out, momentum_out, rms_out, mean_var_out, sem):
    copies = [
        pltpu.make_async_copy(params_ref, params_out, sem.at[0]),
        pltpu.make_async_copy(momentum_ref, momentum_out, sem.at[1]),
        pltpu.make_async_copy(rms_in, rms_out, sem.at[2]),
        pltpu.make_async_copy(mean_var_in, mean_var_out, sem.at[3]),
    ]
    for copy in copies:
        copy.start()
    for copy in copies:
        copy.wait()


def solution(mesh):
    n_rep, n_shard = mesh.shape["rep"], mesh.shape["shard"]

    def shards(delta, counts, params, momentum):
        rows, width = momentum.shape
        full = params.shape[1]
        n_steps = rows // STEP_ROWS
        element_count = rows * width * n_rep * n_shard
        any_space = pl.BlockSpec(memory_space=pl.ANY)
        in_vmem = pl.BlockSpec(memory_space=pltpu.VMEM)
        in_smem = pl.BlockSpec(memory_space=pltpu.SMEM)
        dma = pltpu.SemaphoreType.DMA
        new_params, new_momentum, rms, mean_var = pl.pallas_call(
            functools.partial(kernel, n_rep, n_shard, float(element_count)),
            out_shape=(
                pltpu.VMEM((rows, full), jnp.bfloat16),
                pltpu.VMEM((rows, width), jnp.float32),
                pltpu.SMEM((1,), jnp.float32),
                pltpu.SMEM((1,), jnp.float32),
            ),
            in_specs=[any_space] * 4,
            out_specs=(in_vmem, in_vmem, in_smem, in_smem),
            scratch_shapes=[
                pltpu.VMEM((rows, full), jnp.bfloat16),
                pltpu.VMEM((n_rep - 1, rows, width), jnp.bfloat16),
                pltpu.VMEM((rows, width), jnp.float32),
                pltpu.VMEM((rows, width), jnp.float32),
                pltpu.VMEM((rows, width), jnp.bfloat16),
                pltpu.VMEM((rows, width), jnp.float32),
                pltpu.VMEM((n_rep * n_shard, 1, 128), jnp.float32),
                pltpu.SMEM((n_rep,), jnp.int32),
                dma((n_steps,)),
                dma((3,)),
                dma((n_steps, n_rep - 1)),
                dma((n_steps, n_rep - 1)),
                dma,
                dma,
                dma((n_steps, n_rep - 1)),
                dma((n_steps, n_rep - 1)),
                pltpu.SemaphoreType.REGULAR((n_shard.bit_length() + 1,)),
            ],
            compiler_params=pltpu.CompilerParams(collective_id=0, has_side_effects=True),
        )(delta, counts, params, momentum)
        new_params, new_momentum, rms, mean_var = pl.pallas_call(
            store,
            out_shape=(
                jax.ShapeDtypeStruct((rows, full), jnp.bfloat16),
                jax.ShapeDtypeStruct((rows, width), jnp.float32),
                jax.ShapeDtypeStruct((1,), jnp.float32),
                jax.ShapeDtypeStruct((1,), jnp.float32),
            ),
            in_specs=[any_space, any_space, in_smem, in_smem],
            out_specs=(any_space,) * 4,
            scratch_shapes=[dma((4,))],
        )(
            pltpu.with_memory_space_constraint(new_params, pltpu.VMEM),
            pltpu.with_memory_space_constraint(new_momentum, pltpu.VMEM),
            rms,
            mean_var,
        )
        return new_params, new_momentum, rms.reshape(()), mean_var.reshape(())

    return jax.shard_map(
        shards,
        mesh=mesh,
        in_specs=(P("rep", "shard", None), P(), P("shard", None), P("shard", "rep")),
        out_specs=(P("shard", None), P("shard", "rep"), P(), P()),
        check_vma=False,
    )
```
